256 devices in a mesh: shift: 4 (over x), fsdp: 32 (over z, y_lo, core), tp: 2 (over y_hi).
Axes of the slice: x: 4, y: 4 (y_hi: 2, y_lo: 2; y = y_hi * 2 + y_lo), z: 8, core: 2. Of those that a mesh axis runs over, the one named last changes fastest.
Arguments:
- grad_stack: float32 [512, 128, 2048], P('shift', 'fsdp', 'tp'), parts along dimension 0, may hold values from -6 to 6
- moment_stack: float32 [512, 128, 2048], P('shift', 'fsdp', 'tp'), parts along dimension 0, may hold values from -6 to 6
- weight_stack: float32 [512, 128, 2048], P('shift', 'fsdp', 'tp'), parts along dimension 0, may hold values from -0.1875 to 0.1875
Outputs:
- new_weights: float32 [512, 128, 2048], P('shift', 'fsdp', 'tp'), parts along dimension 0
- new_momentum: float32 [512, 128, 2048], P('shift', 'fsdp', 'tp'), parts along dimension 0
The draws below stay inside these ranges and needn't reach their ends.
There are 4 independent parts, one for each index of `shift`. The reference program is written for one: setup_inputs(seed, part) draws one part's arguments, and reference() takes and returns one part's arrays. A program takes and returns all parts, laid end to end along the dimension named above; each array names one. Nothing has to cross between parts.
All inputs are finite; a program needn't handle non-finite values.
Results may differ from the reference program's by a relative error of at most 0.0003.
Values sent between devices are 32-bit elements.
A program may use at most 64 MiB of HBM per device.

```python
import jax
import jax.numpy as jnp
from jax import lax

SIDE = 128
WIDE = 2048
MATS = 128
ITERS = 3


def block_scale(key, dims, cuts, smallest, largest):
    loudness, own = 1.0, jax.random.fold_in(key, 6)
    for position, parts in cuts:
        draws = jnp.exp(jax.random.uniform(jax.random.fold_in(own, position), (parts,), jnp.float32, smallest / len(cuts), largest / len(cuts)))
        loudness = loudness * jnp.repeat(draws, dims[position] // parts).reshape([-1 if axis == position else 1 for axis in range(len(dims))])
    return loudness


def gaussian(rng, shape, spread, reach, split=(), dtype=jnp.bfloat16):
    factor_of = block_scale(rng, shape, split, -0.22, 0.18) if split else 1.0
    array = jax.random.normal(rng, shape, jnp.float32) * spread * factor_of
    return jnp.minimum(jnp.maximum(array, -reach), reach).astype(dtype)


def setup_inputs(seed: int = 0, part: int = 0) -> dict:
    key_list = jax.random.split(jax.random.key(seed), 4)
    part_splits = jax.random.split(jax.random.fold_in(key_list[3], part), 4)
    grad_stack = gaussian(part_splits[0], (MATS, SIDE, WIDE), 1.0, 6.0, ((1, 32), (2, 2)), jnp.float32)
    moment_stack = gaussian(part_splits[1], (MATS, SIDE, WIDE), 1.0, 6.0, ((1, 32), (2, 2)), jnp.float32)
    weight_stack = gaussian(part_splits[2], (MATS, SIDE, WIDE), 0.03, 0.1875, ((1, 32), (2, 2)), jnp.float32)
    return dict(grad_stack=grad_stack, moment_stack=moment_stack, weight_stack=weight_stack)


hold_rate = 0.95
learn_rate = 0.9

def reference(grad_stack, moment_stack, weight_stack):
    new_momentum = hold_rate * moment_stack + grad_stack

    def orthogonal_one(stack):
        iterate = stack[None]
        iterate = iterate * lax.rsqrt(lax.optimization_barrier(jnp.sum(iterate * iterate, axis=(1, 2), keepdims=True)) + 1e-06)
        for step in range(ITERS):
            gram = jnp.einsum('mik,mjk->mij', iterate, iterate, precision=lax.Precision.HIGHEST)
            mixed = -4.775 * gram + 2.0315 * jnp.einsum('mij,mjk->mik', gram, gram, precision=lax.Precision.HIGHEST)
            iterate = 3.4445 * iterate + jnp.einsum('mij,mjk->mik', mixed, iterate, precision=lax.Precision.HIGHEST)
        return iterate[0]
    iterate = lax.map(orthogonal_one, new_momentum)
    new_weights = weight_stack - learn_rate * iterate
    return (new_weights, new_momentum)
```

```python
import functools

import jax
import jax.numpy as jnp
from jax import lax
from jax.experimental import pallas as pl
from jax.experimental.pallas import tpu as pltpu
from jax.sharding import PartitionSpec as P

ITERS = 3
hold_rate = 0.95
learn_rate = 0.9

MESH = pl.DeviceIdType.MESH
HIGHEST = lax.Precision.HIGHEST
F32 = jnp.float32


def mul(a, b):
    return lax.dot_general(a, b, (((1,), (0,)), ((), ())), precision=HIGHEST, preferred_element_type=F32)


def mul_t(a, b):
    return lax.dot_general(a, b, (((1,), (1,)), ((), ())), precision=HIGHEST, preferred_element_type=F32)


def swap_rows(a, b):
    low = lax.broadcasted_iota(jnp.int32, a.shape, a.ndim - 2) < 4
    return (
        jnp.where(low, a, pltpu.roll(b, 4, a.ndim - 2)),
        jnp.where(low, pltpu.roll(a, 4, a.ndim - 2), b),
    )


def polynomial(gram):
    side = gram.shape[0]
    eye = (
        lax.broadcasted_iota(jnp.int32, gram.shape, 0) == lax.broadcasted_iota(jnp.int32, gram.shape, 1)
    ).astype(F32)
    total = jnp.sum(jnp.sum(gram * eye, axis=1, keepdims=True), axis=0, keepdims=True)
    scale = lax.rsqrt(total + 1e-06)
    gram = (gram * scale) * scale
    factor = None
    for step in range(ITERS):
        now = 3.4445 * eye - 4.775 * gram + 2.0315 * mul(gram, gram)
        if step < ITERS - 1:
            gram = mul(mul(now, gram), now)
        factor = now if factor is None else mul(now, factor)
    return factor * scale


def kernel(n, chunks, grad_hbm, moment_hbm, back, mom, grads, moments, taken, made, wide, gram_own, gram_other,
           load_sem, send_sem, in_sem, gram_send_sem, gram_sem, back_sem):
    me = lax.axis_index("fsdp")
    tp = lax.axis_index("tp")
    peer = 1 - tp

    def loads(m):
        rows = pl.ds(m * n, n)
        return (
            pltpu.make_async_copy(grad_hbm.at[rows], grads.at[rows], load_sem.at[0, m]),
            pltpu.make_async_copy(moment_hbm.at[rows], moments.at[rows], load_sem.at[1, m]),
        )

    for m in range(chunks):
        for copy in loads(m):
            copy.start()

    barrier = pltpu.get_barrier_semaphore()

    def greet(k, carry):
        pl.semaphore_signal(barrier, inc=1, device_id={"fsdp": lax.rem(me + k, n)}, device_id_type=MESH)
        return carry

    lax.fori_loop(1, n, greet, 0)
    pl.semaphore_signal(barrier, inc=1, device_id={"tp": peer}, device_id_type=MESH)

    def momentum(m):
        for copy in loads(m):
            copy.wait()
        rows = pl.ds(m * n, n)
        mom[rows] = hold_rate * moments[rows] + grads[rows]
        taken[m * n + me] = mom[m * n + me]

    momentum(0)
    pl.semaphore_wait(barrier, n)

    def scatter(m):
        def send(to):
            pltpu.make_async_remote_copy(
                src_ref=mom.at[m * n + to], dst_ref=taken.at[m * n + me], send_sem=send_sem, recv_sem=in_sem.at[m],
                device_id={"fsdp": to}, device_id_type=MESH).start()

        def pair(k, carry):
            send(lax.rem(me + n // 2 - k, n))
            send(lax.rem(me + n // 2 + k, n))
            return carry

        send(lax.rem(me + n // 2, n))
        lax.fori_loop(1, n // 2, pair, 0)

    for m in range(chunks):
        if m:
            momentum(m)
        scatter(m)

    def wait_for(buffer, sem, m):
        part = buffer.at[pl.ds(m * n, n - 1)]
        pltpu.make_async_copy(part, part, sem).wait()

    def compute(m, carry):
        wait_for(taken, in_sem.at[m], m)
        for j in range(4):
            block = taken[pl.ds(m * n, n), 8 * j:8 * j + 8, :].reshape(n // 2, 2, 8, 128)
            even, odd = swap_rows(block[:, 0], block[:, 1])
            wide[:, 256 * j:256 * j + 128] = even.reshape(4 * n, 128)
            wide[:, 256 * j + 128:256 * j + 256] = odd.reshape(4 * n, 128)
        gram_own[m] = mul_t(wide[...], wide[...])
        swap = pltpu.make_async_remote_copy(
            src_ref=gram_own.at[m], dst_ref=gram_other.at[m], send_sem=gram_send_sem.at[m], recv_sem=gram_sem.at[m],
            device_id={"tp": peer}, device_id_type=MESH)
        swap.start()
        swap.wait()
        factor = -learn_rate * polynomial(gram_own[m] + gram_other[m])
        for j in range(4):
            both = mul(factor, wide[:, 256 * j:256 * j + 256])
            a, b = swap_rows(both[:, :128].reshape(n // 2, 8, 128), both[:, 128:].reshape(n // 2, 8, 128))
            made[pl.ds(m * n, n), 8 * j:8 * j + 8, :] = jnp.stack([a, b], axis=1).reshape(n, 8, 128)
        back[m * n + me] = made[m * n + me]

        def send(to):
            pltpu.make_async_remote_copy(
                src_ref=made.at[m * n + to], dst_ref=back.at[m * n + me], send_sem=send_sem, recv_sem=back_sem.at[m],
                device_id={"fsdp": to}, device_id_type=MESH).start()

        def pair(k, carry):
            send(lax.rem(me + n // 2 - k, n))
            send(lax.rem(me + n // 2 + k, n))
            return carry

        send(lax.rem(me + n // 2, n))
        lax.fori_loop(1, n // 2, pair, 0)
        return carry

    lax.fori_loop(0, chunks, compute, 0)
    for m in range(chunks):
        wait_for(back, back_sem.at[m], m)
    for m in range(2 * chunks):
        wait_for(taken, send_sem, 0)


def body(grad_stack, moment_stack, weight_stack):
    n = lax.axis_size("fsdp")
    mats, rows, cols = grad_stack.shape
    chunks = mats // n

    def tiles(x):
        return x.reshape(mats, rows, cols // 128, 128).transpose(0, 2, 1, 3).reshape(mats, rows * cols // 128, 128)

    def untiles(x):
        return x.reshape(mats, cols // 128, rows, 128).transpose(0, 2, 1, 3).reshape(mats, rows, cols)

    block = (mats, rows * cols // 128, 128)
    side = n * rows
    dma = pltpu.SemaphoreType.DMA
    back, momentum = pl.pallas_call(
        functools.partial(kernel, n, chunks),
        out_shape=[jax.ShapeDtypeStruct(block, F32)] * 2,
        in_specs=[pl.BlockSpec(memory_space=pltpu.HBM)] * 2,
        out_specs=[pl.BlockSpec(memory_space=pltpu.VMEM)] * 2,
        scratch_shapes=[
            pltpu.VMEM(block, F32), pltpu.VMEM(block, F32), pltpu.VMEM(block, F32), pltpu.VMEM(block, F32),
            pltpu.VMEM((side, cols), F32), pltpu.VMEM((chunks, side, side), F32), pltpu.VMEM((chunks, side, side), F32),
            dma((2, chunks)), dma, dma((chunks,)), dma((chunks,)), dma((chunks,)), dma((chunks,)),
        ],
        compiler_params=pltpu.CompilerParams(collective_id=0, has_side_effects=True, vmem_limit_bytes=32 * 2**20),
    )(tiles(grad_stack), tiles(moment_stack))
    new_weights = weight_stack + untiles(back)
    return (new_weights, untiles(momentum))


def solution(mesh):
    spec = P("shift", "fsdp", "tp")
    return jax.shard_map(body, mesh=mesh, in_specs=(spec,) * 3, out_specs=(spec,) * 2, check_vma=False)
```

```python
import functools

import jax
import jax.numpy as jnp
from jax import lax
from jax.experimental import pallas as pl
from jax.experimental.pallas import tpu as pltpu
from jax.sharding import PartitionSpec as P

ITERS = 3
GROUPS = 8
hold_rate = 0.95
learn_rate = 0.9

MESH = pl.DeviceIdType.MESH
HIGHEST = lax.Precision.HIGHEST
F32 = jnp.float32


def mul(a, b):
    return lax.dot_general(a, b, (((1,), (0,)), ((), ())), precision=HIGHEST, preferred_element_type=F32)


def mul_t(a, b):
    return lax.dot_general(a, b, (((1,), (1,)), ((), ())), precision=HIGHEST, preferred_element_type=F32)


def swap_rows(a, b):
    low = lax.broadcasted_iota(jnp.int32, a.shape, a.ndim - 2) < 4
    return (
        jnp.where(low, a, pltpu.roll(b, 4, a.ndim - 2)),
        jnp.where(low, pltpu.roll(a, 4, a.ndim - 2), b),
    )


def polynomial(gram):
    side = gram.shape[0]
    eye = (
        lax.broadcasted_iota(jnp.int32, gram.shape, 0) == lax.broadcasted_iota(jnp.int32, gram.shape, 1)
    ).astype(F32)
    total = jnp.sum(jnp.sum(gram * eye, axis=1, keepdims=True), axis=0, keepdims=True)
    scale = lax.rsqrt(total + 1e-06)
    gram = (gram * scale) * scale
    factor = None
    for step in range(ITERS):
        now = 3.4445 * eye - 4.775 * gram + 2.0315 * mul(gram, gram)
        if step < ITERS - 1:
            gram = mul(mul(now, gram), now)
        factor = now if factor is None else mul(now, factor)
    return factor * scale


def kernel(n, chunks, grad_hbm, moment_hbm, back, mom, grads, moments, taken, made, wide, gram_own, gram_other,
           load_sem, send_sem, in_sem, gram_send_sem, gram_sem, back_sem,
           round_sem):
    me = lax.axis_index("fsdp")
    tp = lax.axis_index("tp")
    peer = 1 - tp

    def loads(m):
        rows = pl.ds(m * n, n)
        return (
            pltpu.make_async_copy(grad_hbm.at[rows], grads.at[rows], load_sem.at[0, m]),
            pltpu.make_async_copy(moment_hbm.at[rows], moments.at[rows], load_sem.at[1, m]),
        )

    for m in range(chunks):
        for copy in loads(m):
            copy.start()

    group = n // GROUPS
    z, q = me // group, me % group

    def at(dz, dq):
        return lax.rem(z + dz, GROUPS) * group + lax.rem(q + dq, group)

    barrier = pltpu.get_barrier_semaphore()
    for dq in range(group):
        for dz in (1, GROUPS - 1) + ((0,) if dq else ()):
            pl.semaphore_signal(barrier, inc=1, device_id={"fsdp": at(dz, dq)}, device_id_type=MESH)
    pl.semaphore_signal(barrier, inc=1, device_id={"tp": peer}, device_id_type=MESH)

    def momentum(m):
        for copy in loads(m):
            copy.wait()
        rows = pl.ds(m * n, n)
        mom[rows] = hold_rate * moments[rows] + grads[rows]
        taken[m * n + me] = mom[m * n + me]

    def sender(source, target, sem, m):
        def send(dz, dq):
            to = at(dz, dq)
            pltpu.make_async_remote_copy(
                src_ref=source.at[m * n + to], dst_ref=target.at[m * n + me], send_sem=send_sem, recv_sem=sem.at[m],
                device_id={"fsdp": to}, device_id_type=MESH).start()

        def sends(distances, first=0):
            def at_index(dq, carry):
                for dz in distances:
                    send(dz, dq)
                return carry

            lax.fori_loop(first, group, at_index, 0)

        return sends

    momentum(0)
    pl.semaphore_wait(barrier, 3 * group)
    for m in range(chunks):
        if m:
            momentum(m)
        sends = sender(mom, taken, in_sem, m)
        sends((1, GROUPS - 1))
        sends((0,), 1)
    for step in range(3):
        for dz in (1, GROUPS - 1):
            pl.semaphore_signal(round_sem.at[step], inc=1, device_id={"fsdp": at(dz, 0)}, device_id_type=MESH)
        pl.semaphore_wait(round_sem.at[step], 2)
    for m in range(chunks):
        sender(mom, taken, in_sem, m)((3, 5, 4, 2, 6))

    def wait_for(buffer, sem, m):
        part = buffer.at[pl.ds(m * n, n - 1)]
        pltpu.make_async_copy(part, part, sem).wait()

    def compute(m, carry):
        wait_for(taken, in_sem.at[m], m)
        for j in range(4):
            block = taken[pl.ds(m * n, n), 8 * j:8 * j + 8, :].reshape(n // 2, 2, 8, 128)
            even, odd = swap_rows(block[:, 0], block[:, 1])
            wide[:, 256 * j:256 * j + 128] = even.reshape(4 * n, 128)
            wide[:, 256 * j + 128:256 * j + 256] = odd.reshape(4 * n, 128)
        gram_own[m] = mul_t(wide[...], wide[...])
        swap = pltpu.make_async_remote_copy(
            src_ref=gram_own.at[m], dst_ref=gram_other.at[m], send_sem=gram_send_sem.at[m], recv_sem=gram_sem.at[m],
            device_id={"tp": peer}, device_id_type=MESH)
        swap.start()
        swap.wait()
        factor = -learn_rate * polynomial(gram_own[m] + gram_other[m])
        for j in range(4):
            both = mul(factor, wide[:, 256 * j:256 * j + 256])
            a, b = swap_rows(both[:, :128].reshape(n // 2, 8, 128), both[:, 128:].reshape(n // 2, 8, 128))
            made[pl.ds(m * n, n), 8 * j:8 * j + 8, :] = jnp.stack([a, b], axis=1).reshape(n, 8, 128)
        back[m * n + me] = made[m * n + me]

        sends = sender(made, back, back_sem, m)
        sends((3, 5, 4, 2, 6, 1, 7))
        sends((0,), 1)
        return carry

    lax.fori_loop(0, chunks, compute, 0)
    for m in range(chunks):
        wait_for(back, back_sem.at[m], m)
    for m in range(2 * chunks):
        wait_for(taken, send_sem, 0)


def finish(parts, weight, back, mom, weight_out, mom_out, total, sem):
    copies = [pltpu.make_async_copy(mom, mom_out, sem.at[parts])]
    copies[0].start()
    size = weight.shape[0] // parts
    for i in range(parts):
        rows = pl.ds(i * size, size)
        total[rows] = weight[rows] + back[rows]
        copies.append(pltpu.make_async_copy(total.at[rows], weight_out.at[rows], sem.at[i]))
        copies[-1].start()
    for copy in copies:
        copy.wait()


def body(grad_stack, moment_stack, weight_stack):
    n = lax.axis_size("fsdp")
    mats, rows, cols = grad_stack.shape
    chunks = mats // n

    def tiles(x):
        return x.reshape(mats, rows, cols // 128, 128).transpose(0, 2, 1, 3).reshape(mats, rows * cols // 128, 128)

    def untiles(x):
        return x.reshape(mats, cols // 128, rows, 128).transpose(0, 2, 1, 3).reshape(mats, rows, cols)

    block = (mats, rows * cols // 128, 128)
    side = n * rows
    dma = pltpu.SemaphoreType.DMA
    back, momentum = pl.pallas_call(
        functools.partial(kernel, n, chunks),
        out_shape=[jax.ShapeDtypeStruct(block, F32)] * 2,
        in_specs=[pl.BlockSpec(memory_space=pltpu.HBM)] * 2,
        out_specs=[pl.BlockSpec(memory_space=pltpu.VMEM)] * 2,
        scratch_shapes=[
            pltpu.VMEM(block, F32), pltpu.VMEM(block, F32), pltpu.VMEM(block, F32), pltpu.VMEM(block, F32),
            pltpu.VMEM((side, cols), F32), pltpu.VMEM((chunks, side, side), F32), pltpu.VMEM((chunks, side, side), F32),
            dma((2, chunks)), dma, dma((chunks,)), dma((chunks,)), dma((chunks,)), dma((chunks,)),
            pltpu.SemaphoreType.REGULAR((3,)),
        ],
        compiler_params=pltpu.CompilerParams(collective_id=0, has_side_effects=True, vmem_limit_bytes=32 * 2**20),
    )(*(pltpu.with_memory_space_constraint(tiles(x), pltpu.HBM) for x in (grad_stack, moment_stack)))
    new_weights, new_momentum = pl.pallas_call(
        functools.partial(finish, 4),
        out_shape=[jax.ShapeDtypeStruct(block, F32)] * 2,
        in_specs=[pl.BlockSpec(memory_space=pltpu.VMEM)] * 3,
        out_specs=[pl.BlockSpec(memory_space=pl.ANY)] * 2,
        scratch_shapes=[pltpu.VMEM(block, F32), dma((5,))],
        compiler_params=pltpu.CompilerParams(vmem_limit_bytes=8 * 2**20),
    )(tiles(weight_stack), back, momentum)
    return (untiles(new_weights), untiles(new_momentum))


def solution(mesh):
    spec = P("shift", "fsdp", "tp")
    return jax.shard_map(body, mesh=mesh, in_specs=(spec,) * 3, out_specs=(spec,) * 2, check_vma=False)
```

```python
import functools

import jax
import jax.numpy as jnp
from jax import lax
from jax.experimental import pallas as pl
from jax.experimental.pallas import tpu as pltpu
from jax.sharding import PartitionSpec as P

ITERS = 3
DEPTH = 8
GROUP = 4
hold_rate = 0.95
learn_rate = 0.9

MESH = pl.DeviceIdType.MESH
HIGHEST = lax.Precision.HIGHEST
F32 = jnp.float32


OWN, BESIDE, ACROSS, OBLIQUE, FIRST, SECOND, THIRD, FOURTH = range(8)
ROW, NEXT, TURNS = (OWN, BESIDE), (ACROSS, OBLIQUE), (FIRST, SECOND, THIRD, FOURTH)
ZERO = ((0, BESIDE), (0, ACROSS), (0, OBLIQUE))


def moves(distances, places):
    return tuple((dz, place) for place in places for dz in distances)


OUT = ZERO + moves((4,), TURNS) + moves((3, 5), TURNS) + moves((2, 6), TURNS) + moves((1, 7), TURNS)
LAST = ((0, 4), (4, 8), (8, 32))


def mul(a, b):
    return lax.dot_general(a, b, (((1,), (0,)), ((), ())), precision=HIGHEST, preferred_element_type=F32)


def mul_t(a, b):
    return lax.dot_general(a, b, (((1,), (1,)), ((), ())), precision=HIGHEST, preferred_element_type=F32)


def swap_rows(a, b):
    low = lax.broadcasted_iota(jnp.int32, a.shape, a.ndim - 2) < 4
    return (
        jnp.where(low, a, pltpu.roll(b, 4, a.ndim - 2)),
        jnp.where(low, pltpu.roll(a, 4, a.ndim - 2), b),
    )


def polynomial(gram):
    side = gram.shape[0]
    eye = (
        lax.broadcasted_iota(jnp.int32, gram.shape, 0) == lax.broadcasted_iota(jnp.int32, gram.shape, 1)
    ).astype(F32)
    total = jnp.sum(jnp.sum(gram * eye, axis=1, keepdims=True), axis=0, keepdims=True)
    scale = lax.rsqrt(total + 1e-06)
    gram = (gram * scale) * scale
    factor = None
    for step in range(ITERS):
        now = 3.4445 * eye - 4.775 * gram + 2.0315 * mul(gram, gram)
        if step < ITERS - 1:
            gram = mul(mul(now, gram), now)
        factor = now if factor is None else mul(now, factor)
    return factor * scale


def kernel(n, chunks, grad_hbm, moment_hbm, back, mom, grads, moments, taken, made, wide, gram_own, gram_other,
           load_sem, send_sem, in_sem, gram_send_sem, gram_sem, back_sem,
           round_sem):
    me = lax.axis_index("fsdp")
    tp = lax.axis_index("tp")
    peer = 1 - tp

    def loads(m):
        rows = pl.ds(m * n, n)
        return (
            pltpu.make_async_copy(grad_hbm.at[rows], grads.at[rows], load_sem.at[0, m]),
            pltpu.make_async_copy(moment_hbm.at[rows], moments.at[rows], load_sem.at[1, m]),
        )

    for m in range(chunks):
        for copy in loads(m):
            copy.start()

    z, q = me // GROUP, me % GROUP
    odd = q % 2
    places = {OWN: 0, BESIDE: 1 + 2 * odd, ACROSS: 2, OBLIQUE: 3 - 2 * odd,
              FIRST: 2 * odd, SECOND: 2 - 2 * odd, THIRD: 1, FOURTH: 3}

    def at(dz, place):
        return lax.rem(z + dz, DEPTH) * GROUP + lax.rem(q + places[place], GROUP)

    barrier = pltpu.get_barrier_semaphore()
    greeted = moves((1, DEPTH - 1), TURNS) + ZERO
    for shift in greeted:
        pl.semaphore_signal(barrier, inc=1, device_id={"fsdp": at(*shift)}, device_id_type=MESH)
    pl.semaphore_signal(barrier, inc=1, device_id={"tp": peer}, device_id_type=MESH)

    def momentum(m):
        for copy in loads(m):
            copy.wait()
        rows = pl.ds(m * n, n)
        mom[rows] = hold_rate * moments[rows] + grads[rows]
        taken[m * n + me] = mom[m * n + me]

    def send(source, target, sem, m, to_shifts):
        for shift in to_shifts:
            to = at(*shift)
            pltpu.make_async_remote_copy(
                src_ref=source.at[m * n + to], dst_ref=target.at[m * n + me], send_sem=send_sem, recv_sem=sem.at[m],
                device_id={"fsdp": to}, device_id_type=MESH).start()

    def send_some(source, target, sem, m, to_moves, low, high):
        for move in to_moves:
            to = at(*move)

            @pl.when((to >= low) & (to < high))
            def _():
                pltpu.make_async_remote_copy(
                    src_ref=source.at[m * n + to], dst_ref=target.at[m * n + me], send_sem=send_sem,
                    recv_sem=sem.at[m], device_id={"fsdp": to}, device_id_type=MESH).start()

    def scatter(first, last, to_shifts):
        def one(m, carry):
            send(mom, taken, in_sem, m, to_shifts)
            return carry

        lax.fori_loop(first, last, one, 0)

    def round_of(step):
        for dz in (1, DEPTH - 1):
            pl.semaphore_signal(round_sem.at[step], inc=1, device_id={"fsdp": at(dz, OWN)}, device_id_type=MESH)
        pl.semaphore_wait(round_sem.at[step], 2)

    momentum(0)
    pl.semaphore_wait(barrier, len(greeted) + 1)
    for m in range(chunks):
        if m:
            momentum(m)
        send(mom, taken, in_sem, m, moves((1, 7), ROW) + ZERO)
    round_of(0)
    scatter(0, chunks, moves((2, 6), ROW))
    round_of(1)
    round_of(2)
    scatter(0, chunks, moves((4, 3, 5), TURNS) + moves((2, 6, 1, 7), NEXT))
    def wait_for(buffer, sem, m):
        part = buffer.at[pl.ds(m * n, n - 1)]
        pltpu.make_async_copy(part, part, sem).wait()

    def compute(m, carry):
        wait_for(taken, in_sem.at[m], m)
        for j in range(4):
            block = taken[pl.ds(m * n, n), 8 * j:8 * j + 8, :].reshape(n // 2, 2, 8, 128)
            even, odd = swap_rows(block[:, 0], block[:, 1])
            wide[:, 256 * j:256 * j + 128] = even.reshape(4 * n, 128)
            wide[:, 256 * j + 128:256 * j + 256] = odd.reshape(4 * n, 128)
        gram_own[m] = mul_t(wide[...], wide[...])
        swap = pltpu.make_async_remote_copy(
            src_ref=gram_own.at[m], dst_ref=gram_other.at[m], send_sem=gram_send_sem.at[m], recv_sem=gram_sem.at[m],
            device_id={"tp": peer}, device_id_type=MESH)
        swap.start()
        swap.wait()
        factor = -learn_rate * polynomial(gram_own[m] + gram_other[m])
        for j in range(4):
            both = mul(factor, wide[:, 256 * j:256 * j + 256])
            a, b = swap_rows(both[:, :128].reshape(n // 2, 8, 128), both[:, 128:].reshape(n // 2, 8, 128))
            made[pl.ds(m * n, n), 8 * j:8 * j + 8, :] = jnp.stack([a, b], axis=1).reshape(n, 8, 128)
        back[m * n + me] = made[m * n + me]

        @pl.when(m < chunks - 1)
        def _():
            send(made, back, back_sem, m, OUT)

        @pl.when(m == chunks - 1)
        def _():
            for low, high in LAST:
                send_some(made, back, back_sem, m, OUT, low, high)

        return carry

    lax.fori_loop(0, chunks, compute, 0)
    for m in range(chunks):
        wait_for(back, back_sem.at[m], m)
    for m in range(2 * chunks):
        wait_for(taken, send_sem, 0)


def finish(parts, weight, back, mom, weight_out, mom_out, total, sem):
    copies = [pltpu.make_async_copy(mom, mom_out, sem.at[parts])]
    copies[0].start()
    size = weight.shape[0] // parts
    for i in range(parts):
        rows = pl.ds(i * size, size)
        total[rows] = weight[rows] + back[rows]
        copies.append(pltpu.make_async_copy(total.at[rows], weight_out.at[rows], sem.at[i]))
        copies[-1].start()
    for copy in copies:
        copy.wait()


def body(grad_stack, moment_stack, weight_stack):
    n = lax.axis_size("fsdp")
    mats, rows, cols = grad_stack.shape
    chunks = mats // n

    def tiles(x):
        return x.reshape(mats, rows, cols // 128, 128).transpose(0, 2, 1, 3).reshape(mats, rows * cols // 128, 128)

    def untiles(x):
        return x.reshape(mats, cols // 128, rows, 128).transpose(0, 2, 1, 3).reshape(mats, rows, cols)

    block = (mats, rows * cols // 128, 128)
    side = n * rows
    dma = pltpu.SemaphoreType.DMA
    back, momentum = pl.pallas_call(
        functools.partial(kernel, n, chunks),
        out_shape=[jax.ShapeDtypeStruct(block, F32)] * 2,
        in_specs=[pl.BlockSpec(memory_space=pltpu.HBM)] * 2,
        out_specs=[pl.BlockSpec(memory_space=pltpu.VMEM)] * 2,
        scratch_shapes=[
            pltpu.VMEM(block, F32), pltpu.VMEM(block, F32), pltpu.VMEM(block, F32), pltpu.VMEM(block, F32),
            pltpu.VMEM((side, cols), F32), pltpu.VMEM((chunks, side, side), F32), pltpu.VMEM((chunks, side, side), F32),
            dma((2, chunks)), dma, dma((chunks,)), dma((chunks,)), dma((chunks,)), dma((chunks,)),
            pltpu.SemaphoreType.REGULAR((3,)),
        ],
        compiler_params=pltpu.CompilerParams(collective_id=0, has_side_effects=True, vmem_limit_bytes=32 * 2**20),
    )(*(pltpu.with_memory_space_constraint(tiles(x), pltpu.HBM) for x in (grad_stack, moment_stack)))
    new_weights, new_momentum = pl.pallas_call(
        functools.partial(finish, 4),
        out_shape=[jax.ShapeDtypeStruct(block, F32)] * 2,
        in_specs=[pl.BlockSpec(memory_space=pltpu.VMEM)] * 3,
        out_specs=[pl.BlockSpec(memory_space=pl.ANY)] * 2,
        scratch_shapes=[pltpu.VMEM(block, F32), dma((5,))],
        compiler_params=pltpu.CompilerParams(vmem_limit_bytes=8 * 2**20),
    )(tiles(weight_stack), back, momentum)
    return (untiles(new_weights), untiles(new_momentum))


def solution(mesh):
    spec = P("shift", "fsdp", "tp")
    return jax.shard_map(body, mesh=mesh, in_specs=(spec,) * 3, out_specs=(spec,) * 2, check_vma=False)
```

```python
import functools

import jax
import jax.numpy as jnp
from jax import lax
from jax.experimental import pallas as pl
from jax.experimental.pallas import tpu as pltpu
from jax.sharding import PartitionSpec as P

ITERS = 3
DEPTH = 8
GROUP = 4
hold_rate = 0.95
learn_rate = 0.9

MESH = pl.DeviceIdType.MESH
HIGHEST = lax.Precision.HIGHEST
F32 = jnp.float32


OWN, BESIDE, ACROSS, OBLIQUE, FIRST, SECOND, THIRD, FOURTH = range(8)
ROW, NEXT, TURNS = (OWN, BESIDE), (ACROSS, OBLIQUE), (FIRST, SECOND, THIRD, FOURTH)
ZERO = ((0, BESIDE), (0, ACROSS), (0, OBLIQUE))


def moves(distances, places):
    return tuple((dz, place) for place in places for dz in distances)


OUT = ZERO + moves((4,), TURNS) + moves((5, 3), TURNS) + moves((6, 2), TURNS) + moves((7, 1), TURNS)
LAST = ((0, 4), (4, 8), (8, 32))


def mul(a, b):
    return lax.dot_general(a, b, (((1,), (0,)), ((), ())), precision=HIGHEST, preferred_element_type=F32)


def mul_t(a, b):
    return lax.dot_general(a, b, (((1,), (1,)), ((), ())), precision=HIGHEST, preferred_element_type=F32)


def swap_rows(a, b):
    low = lax.broadcasted_iota(jnp.int32, a.shape, a.ndim - 2) < 4
    return (
        jnp.where(low, a, pltpu.roll(b, 4, a.ndim - 2)),
        jnp.where(low, pltpu.roll(a, 4, a.ndim - 2), b),
    )


def polynomial(gram):
    side = gram.shape[0]
    eye = (
        lax.broadcasted_iota(jnp.int32, gram.shape, 0) == lax.broadcasted_iota(jnp.int32, gram.shape, 1)
    ).astype(F32)
    total = jnp.sum(jnp.sum(gram * eye, axis=1, keepdims=True), axis=0, keepdims=True)
    scale = lax.rsqrt(total + 1e-06)
    gram = (gram * scale) * scale
    factor = None
    for step in range(ITERS):
        now = 3.4445 * eye - 4.775 * gram + 2.0315 * mul(gram, gram)
        if step < ITERS - 1:
            gram = mul(mul(now, gram), now)
        factor = now if factor is None else mul(now, factor)
    return factor * scale


def kernel(n, chunks, grad_hbm, moment_hbm, back, mom, grads, moments, taken, made, wide, gram_own, gram_other,
           load_sem, send_sem, in_sem, gram_send_sem, gram_sem, back_sem,
           round_sem):
    me = lax.axis_index("fsdp")
    tp = lax.axis_index("tp")
    peer = 1 - tp

    def loads(m):
        rows = pl.ds(m * n, n)
        return (
            pltpu.make_async_copy(grad_hbm.at[rows], grads.at[rows], load_sem.at[0, m]),
            pltpu.make_async_copy(moment_hbm.at[rows], moments.at[rows], load_sem.at[1, m]),
        )

    for m in range(chunks):
        for copy in loads(m):
            copy.start()

    z, q = me // GROUP, me % GROUP
    odd = q % 2
    places = {OWN: 0, BESIDE: 1 + 2 * odd, ACROSS: 2, OBLIQUE: 3 - 2 * odd,
              FIRST: 2 * odd, SECOND: 2 - 2 * odd, THIRD: 1, FOURTH: 3}

    def at(dz, place):
        return lax.rem(z + dz, DEPTH) * GROUP + lax.rem(q + places[place], GROUP)

    barrier = pltpu.get_barrier_semaphore()
    greeted = moves((1, DEPTH - 1), TURNS) + ZERO
    for shift in greeted:
        pl.semaphore_signal(barrier, inc=1, device_id={"fsdp": at(*shift)}, device_id_type=MESH)
    pl.semaphore_signal(barrier, inc=1, device_id={"tp": peer}, device_id_type=MESH)

    def momentum(m):
        for copy in loads(m):
            copy.wait()
        rows = pl.ds(m * n, n)
        mom[rows] = hold_rate * moments[rows] + grads[rows]
        taken[m * n + me] = mom[m * n + me]

    def send(source, target, sem, m, to_shifts):
        for shift in to_shifts:
            to = at(*shift)
            pltpu.make_async_remote_copy(
                src_ref=source.at[m * n + to], dst_ref=target.at[m * n + me], send_sem=send_sem, recv_sem=sem.at[m],
                device_id={"fsdp": to}, device_id_type=MESH).start()

    def send_some(source, target, sem, m, to_moves, low, high):
        for move in to_moves:
            to = at(*move)

            @pl.when((to >= low) & (to < high))
            def _():
                pltpu.make_async_remote_copy(
                    src_ref=source.at[m * n + to], dst_ref=target.at[m * n + me], send_sem=send_sem,
                    recv_sem=sem.at[m], device_id={"fsdp": to}, device_id_type=MESH).start()

    def scatter(first, last, to_shifts):
        def one(m, carry):
            send(mom, taken, in_sem, m, to_shifts)
            return carry

        lax.fori_loop(first, last, one, 0)

    def round_of(step):
        for dz in (1, DEPTH - 1):
            pl.semaphore_signal(round_sem.at[step], inc=1, device_id={"fsdp": at(dz, OWN)}, device_id_type=MESH)
        pl.semaphore_wait(round_sem.at[step], 2)

    momentum(0)
    pl.semaphore_wait(barrier, len(greeted) + 1)
    for m in range(chunks):
        if m:
            momentum(m)
        send(mom, taken, in_sem, m, moves((1, 7), ROW) + ZERO)
    round_of(0)
    scatter(0, chunks, moves((2, 6), ROW))
    round_of(1)
    round_of(2)
    scatter(0, chunks, moves((4, 3, 5), TURNS) + moves((2, 6, 1, 7), NEXT))
    def wait_for(buffer, sem, m):
        part = buffer.at[pl.ds(m * n, n - 1)]
        pltpu.make_async_copy(part, part, sem).wait()

    def compute(m, carry):
        wait_for(taken, in_sem.at[m], m)
        for j in range(4):
            block = taken[pl.ds(m * n, n), 8 * j:8 * j + 8, :].reshape(n // 2, 2, 8, 128)
            even, odd = swap_rows(block[:, 0], block[:, 1])
            wide[:, 256 * j:256 * j + 128] = even.reshape(4 * n, 128)
            wide[:, 256 * j + 128:256 * j + 256] = odd.reshape(4 * n, 128)
        gram_own[m] = mul_t(wide[...], wide[...])
        swap = pltpu.make_async_remote_copy(
            src_ref=gram_own.at[m], dst_ref=gram_other.at[m], send_sem=gram_send_sem.at[m], recv_sem=gram_sem.at[m],
            device_id={"tp": peer}, device_id_type=MESH)
        swap.start()
        swap.wait()
        factor = -learn_rate * polynomial(gram_own[m] + gram_other[m])
        for j in range(4):
            both = mul(factor, wide[:, 256 * j:256 * j + 256])
            a, b = swap_rows(both[:, :128].reshape(n // 2, 8, 128), both[:, 128:].reshape(n // 2, 8, 128))
            made[pl.ds(m * n, n), 8 * j:8 * j + 8, :] = jnp.stack([a, b], axis=1).reshape(n, 8, 128)
        back[m * n + me] = made[m * n + me]

        @pl.when(m < chunks - 1)
        def _():
            send(made, back, back_sem, m, OUT)

        @pl.when(m == chunks - 1)
        def _():
            for low, high in LAST:
                send_some(made, back, back_sem, m, OUT, low, high)

        return carry

    lax.fori_loop(0, chunks, compute, 0)
    for m in range(chunks):
        wait_for(back, back_sem.at[m], m)
    for m in range(2 * chunks):
        wait_for(taken, send_sem, 0)


def finish(parts, weight, back, mom, weight_out, mom_out, total, sem):
    copies = [pltpu.make_async_copy(mom, mom_out, sem.at[parts])]
    copies[0].start()
    size = weight.shape[0] // parts
    for i in range(parts):
        rows = pl.ds(i * size, size)
        total[rows] = weight[rows] + back[rows]
        copies.append(pltpu.make_async_copy(total.at[rows], weight_out.at[rows], sem.at[i]))
        copies[-1].start()
    for copy in copies:
        copy.wait()


def body(grad_stack, moment_stack, weight_stack):
    n = lax.axis_size("fsdp")
    mats, rows, cols = grad_stack.shape
    chunks = mats // n

    def tiles(x):
        return x.reshape(mats, rows, cols // 128, 128).transpose(0, 2, 1, 3).reshape(mats, rows * cols // 128, 128)

    def untiles(x):
        return x.reshape(mats, cols // 128, rows, 128).transpose(0, 2, 1, 3).reshape(mats, rows, cols)

    block = (mats, rows * cols // 128, 128)
    side = n * rows
    dma = pltpu.SemaphoreType.DMA
    back, momentum = pl.pallas_call(
        functools.partial(kernel, n, chunks),
        out_shape=[jax.ShapeDtypeStruct(block, F32)] * 2,
        in_specs=[pl.BlockSpec(memory_space=pltpu.HBM)] * 2,
        out_specs=[pl.BlockSpec(memory_space=pltpu.VMEM)] * 2,
        scratch_shapes=[
            pltpu.VMEM(block, F32), pltpu.VMEM(block, F32), pltpu.VMEM(block, F32), pltpu.VMEM(block, F32),
            pltpu.VMEM((side, cols), F32), pltpu.VMEM((chunks, side, side), F32), pltpu.VMEM((chunks, side, side), F32),
            dma((2, chunks)), dma, dma((chunks,)), dma((chunks,)), dma((chunks,)), dma((chunks,)),
            pltpu.SemaphoreType.REGULAR((3,)),
        ],
        compiler_params=pltpu.CompilerParams(collective_id=0, has_side_effects=True, vmem_limit_bytes=32 * 2**20),
    )(*(pltpu.with_memory_space_constraint(tiles(x), pltpu.HBM) for x in (grad_stack, moment_stack)))
    new_weights, new_momentum = pl.pallas_call(
        functools.partial(finish, 4),
        out_shape=[jax.ShapeDtypeStruct(block, F32)] * 2,
        in_specs=[pl.BlockSpec(memory_space=pltpu.VMEM)] * 3,
        out_specs=[pl.BlockSpec(memory_space=pl.ANY)] * 2,
        scratch_shapes=[pltpu.VMEM(block, F32), dma((5,))],
        compiler_params=pltpu.CompilerParams(vmem_limit_bytes=8 * 2**20),
    )(tiles(weight_stack), back, momentum)
    return (untiles(new_weights), untiles(new_momentum))


def solution(mesh):
    spec = P("shift", "fsdp", "tp")
    return jax.shard_map(body, mesh=mesh, in_specs=(spec,) * 3, out_specs=(spec,) * 2, check_vma=False)
```

```python
import functools

import jax
import jax.numpy as jnp
from jax import lax
from jax.experimental import pallas as pl
from jax.experimental.pallas import tpu as pltpu
from jax.sharding import PartitionSpec as P

ITERS = 3
DEPTH = 8
GROUP = 4
hold_rate = 0.95
learn_rate = 0.9

MESH = pl.DeviceIdType.MESH
HIGHEST = lax.Precision.HIGHEST
F32 = jnp.float32


OWN, BESIDE, ACROSS, OBLIQUE, FIRST, SECOND, THIRD, FOURTH = range(8)
ROW, NEXT, TURNS = (OWN, BESIDE), (ACROSS, OBLIQUE), (FIRST, SECOND, THIRD, FOURTH)
ZERO = ((0, BESIDE), (0, ACROSS), (0, OBLIQUE))


def moves(distances, places):
    return tuple((dz, place) for place in places for dz in distances)


OUT = ZERO + moves((4,), TURNS) + moves((5, 3), TURNS) + moves((6, 2), TURNS) + moves((7, 1), TURNS)
LAST = ((0, 4), (4, 8), (8, 32))


def mul(a, b):
    return lax.dot_general(a, b, (((1,), (0,)), ((), ())), precision=HIGHEST, preferred_element_type=F32)


def mul_t(a, b):
    return lax.dot_general(a, b, (((1,), (1,)), ((), ())), precision=HIGHEST, preferred_element_type=F32)


def swap_rows(a, b):
    low = lax.broadcasted_iota(jnp.int32, a.shape, a.ndim - 2) < 4
    return (
        jnp.where(low, a, pltpu.roll(b, 4, a.ndim - 2)),
        jnp.where(low, pltpu.roll(a, 4, a.ndim - 2), b),
    )


def polynomial(gram):
    side = gram.shape[0]
    eye = (
        lax.broadcasted_iota(jnp.int32, gram.shape, 0) == lax.broadcasted_iota(jnp.int32, gram.shape, 1)
    ).astype(F32)
    total = jnp.sum(jnp.sum(gram * eye, axis=1, keepdims=True), axis=0, keepdims=True)
    scale = lax.rsqrt(total + 1e-06)
    gram = (gram * scale) * scale
    factor = None
    for step in range(ITERS):
        now = 3.4445 * eye - 4.775 * gram + 2.0315 * mul(gram, gram)
        if step < ITERS - 1:
            gram = mul(mul(now, gram), now)
        factor = now if factor is None else mul(now, factor)
    return factor * scale


def kernel(n, chunks, grad_hbm, moment_hbm, back, mom, grads, moments, taken, made, wide, gram_own, gram_other,
           load_sem, send_sem, in_sem, gram_send_sem, gram_sem, back_sem,
           round_sem):
    me = lax.axis_index("fsdp")
    tp = lax.axis_index("tp")
    peer = 1 - tp

    def loads(m):
        rows = pl.ds(m * n, n)
        return (
            pltpu.make_async_copy(grad_hbm.at[rows], grads.at[rows], load_sem.at[0, m]),
            pltpu.make_async_copy(moment_hbm.at[rows], moments.at[rows], load_sem.at[1, m]),
        )

    for m in range(chunks):
        for copy in loads(m):
            copy.start()

    z, q = me // GROUP, me % GROUP
    odd = q % 2
    places = {OWN: 0, BESIDE: 1 + 2 * odd, ACROSS: 2, OBLIQUE: 3 - 2 * odd,
              FIRST: 2 * odd, SECOND: 2 - 2 * odd, THIRD: 1, FOURTH: 3}

    def at(dz, place):
        return lax.rem(z + dz, DEPTH) * GROUP + lax.rem(q + places[place], GROUP)

    barrier = pltpu.get_barrier_semaphore()
    greeted = moves((1, DEPTH - 1), ROW) + ((0, BESIDE), (0, ACROSS))
    for shift in greeted:
        pl.semaphore_signal(barrier, inc=1, device_id={"fsdp": at(*shift)}, device_id_type=MESH)
    pl.semaphore_signal(barrier, inc=1, device_id={"tp": peer}, device_id_type=MESH)

    def momentum(m):
        for copy in loads(m):
            copy.wait()
        rows = pl.ds(m * n, n)
        mom[rows] = hold_rate * moments[rows] + grads[rows]
        taken[m * n + me] = mom[m * n + me]

    def send(source, target, sem, m, to_shifts):
        for shift in to_shifts:
            to = at(*shift)
            pltpu.make_async_remote_copy(
                src_ref=source.at[m * n + to], dst_ref=target.at[m * n + me], send_sem=send_sem, recv_sem=sem.at[m],
                device_id={"fsdp": to}, device_id_type=MESH).start()

    def send_some(source, target, sem, m, to_moves, low, high):
        for move in to_moves:
            to = at(*move)

            @pl.when((to >= low) & (to < high))
            def _():
                pltpu.make_async_remote_copy(
                    src_ref=source.at[m * n + to], dst_ref=target.at[m * n + me], send_sem=send_sem,
                    recv_sem=sem.at[m], device_id={"fsdp": to}, device_id_type=MESH).start()

    def scatter(first, last, to_shifts):
        def one(m, carry):
            send(mom, taken, in_sem, m, to_shifts)
            return carry

        lax.fori_loop(first, last, one, 0)

    def round_of(step):
        told = ((1, OWN), (DEPTH - 1, OWN)) + (((0, ACROSS),) if step == 0 else ())
        for move in told:
            pl.semaphore_signal(round_sem.at[step], inc=1, device_id={"fsdp": at(*move)}, device_id_type=MESH)
        pl.semaphore_wait(round_sem.at[step], len(told))

    momentum(0)
    pl.semaphore_wait(barrier, len(greeted) + 1)
    for m in range(chunks):
        if m:
            momentum(m)
        send(mom, taken, in_sem, m, moves((1, 7), ROW) + ((0, BESIDE), (0, ACROSS)))
    round_of(0)
    scatter(0, chunks, moves((2, 6), ROW) + ((0, OBLIQUE),))
    round_of(1)
    round_of(2)
    round_of(3)
    scatter(0, chunks, moves((4, 3, 5), TURNS) + moves((2, 6, 1, 7), NEXT))
    def wait_for(buffer, sem, m):
        part = buffer.at[pl.ds(m * n, n - 1)]
        pltpu.make_async_copy(part, part, sem).wait()

    def compute(m, carry):
        wait_for(taken, in_sem.at[m], m)
        for j in range(4):
            block = taken[pl.ds(m * n, n), 8 * j:8 * j + 8, :].reshape(n // 2, 2, 8, 128)
            even, odd = swap_rows(block[:, 0], block[:, 1])
            wide[:, 256 * j:256 * j + 128] = even.reshape(4 * n, 128)
            wide[:, 256 * j + 128:256 * j + 256] = odd.reshape(4 * n, 128)
        gram_own[m] = mul_t(wide[...], wide[...])
        swap = pltpu.make_async_remote_copy(
            src_ref=gram_own.at[m], dst_ref=gram_other.at[m], send_sem=gram_send_sem.at[m], recv_sem=gram_sem.at[m],
            device_id={"tp": peer}, device_id_type=MESH)
        swap.start()
        swap.wait()
        factor = -learn_rate * polynomial(gram_own[m] + gram_other[m])
        for j in range(4):
            both = mul(factor, wide[:, 256 * j:256 * j + 256])
            a, b = swap_rows(both[:, :128].reshape(n // 2, 8, 128), both[:, 128:].reshape(n // 2, 8, 128))
            made[pl.ds(m * n, n), 8 * j:8 * j + 8, :] = jnp.stack([a, b], axis=1).reshape(n, 8, 128)
        back[m * n + me] = made[m * n + me]

        @pl.when(m < chunks - 1)
        def _():
            send(made, back, back_sem, m, OUT)

        @pl.when(m == chunks - 1)
        def _():
            for low, high in LAST:
                send_some(made, back, back_sem, m, OUT, low, high)

        return carry

    lax.fori_loop(0, chunks, compute, 0)
    for m in range(chunks):
        wait_for(back, back_sem.at[m], m)
    for m in range(2 * chunks):
        wait_for(taken, send_sem, 0)


def finish(parts, weight, back, mom, weight_out, mom_out, total, sem):
    copies = [pltpu.make_async_copy(mom, mom_out, sem.at[parts])]
    copies[0].start()
    size = weight.shape[0] // parts
    for i in range(parts):
        rows = pl.ds(i * size, size)
        total[rows] = weight[rows] + back[rows]
        copies.append(pltpu.make_async_copy(total.at[rows], weight_out.at[rows], sem.at[i]))
        copies[-1].start()
    for copy in copies:
        copy.wait()


def body(grad_stack, moment_stack, weight_stack):
    n = lax.axis_size("fsdp")
    mats, rows, cols = grad_stack.shape
    chunks = mats // n

    def tiles(x):
        return x.reshape(mats, rows, cols // 128, 128).transpose(0, 2, 1, 3).reshape(mats, rows * cols // 128, 128)

    def untiles(x):
        return x.reshape(mats, cols // 128, rows, 128).transpose(0, 2, 1, 3).reshape(mats, rows, cols)

    block = (mats, rows * cols // 128, 128)
    side = n * rows
    dma = pltpu.SemaphoreType.DMA
    back, momentum = pl.pallas_call(
        functools.partial(kernel, n, chunks),
        out_shape=[jax.ShapeDtypeStruct(block, F32)] * 2,
        in_specs=[pl.BlockSpec(memory_space=pltpu.HBM)] * 2,
        out_specs=[pl.BlockSpec(memory_space=pltpu.VMEM)] * 2,
        scratch_shapes=[
            pltpu.VMEM(block, F32), pltpu.VMEM(block, F32), pltpu.VMEM(block, F32), pltpu.VMEM(block, F32),
            pltpu.VMEM((side, cols), F32), pltpu.VMEM((chunks, side, side), F32), pltpu.VMEM((chunks, side, side), F32),
            dma((2, chunks)), dma, dma((chunks,)), dma((chunks,)), dma((chunks,)), dma((chunks,)),
            pltpu.SemaphoreType.REGULAR((4,)),
        ],
        compiler_params=pltpu.CompilerParams(collective_id=0, has_side_effects=True, vmem_limit_bytes=32 * 2**20),
    )(*(pltpu.with_memory_space_constraint(tiles(x), pltpu.HBM) for x in (grad_stack, moment_stack)))
    new_weights, new_momentum = pl.pallas_call(
        functools.partial(finish, 4),
        out_shape=[jax.ShapeDtypeStruct(block, F32)] * 2,
        in_specs=[pl.BlockSpec(memory_space=pltpu.VMEM)] * 3,
        out_specs=[pl.BlockSpec(memory_space=pl.ANY)] * 2,
        scratch_shapes=[pltpu.VMEM(block, F32), dma((5,))],
        compiler_params=pltpu.CompilerParams(vmem_limit_bytes=8 * 2**20),
    )(tiles(weight_stack), back, momentum)
    return (untiles(new_weights), untiles(new_momentum))


def solution(mesh):
    spec = P("shift", "fsdp", "tp")
    return jax.shard_map(body, mesh=mesh, in_specs=(spec,) * 3, out_specs=(spec,) * 2, check_vma=False)
```

```python
import functools

import jax
import jax.numpy as jnp
from jax import lax
from jax.experimental import pallas as pl
from jax.experimental.pallas import tpu as pltpu
from jax.sharding import PartitionSpec as P

ITERS = 3
DEPTH = 8
GROUP = 4
hold_rate = 0.95
learn_rate = 0.9

MESH = pl.DeviceIdType.MESH
HIGHEST = lax.Precision.HIGHEST
F32 = jnp.float32


OWN, BESIDE, ACROSS, OBLIQUE, FIRST, SECOND, THIRD, FOURTH = range(8)
ROW, NEXT, TURNS = (OWN, BESIDE), (ACROSS, OBLIQUE), (FIRST, SECOND, THIRD, FOURTH)
ZERO = ((0, BESIDE), (0, ACROSS), (0, OBLIQUE))


def moves(distances, places):
    return tuple((dz, place) for place in places for dz in distances)


OUT = ZERO + moves((4,), TURNS) + moves((5, 3), TURNS) + moves((6, 2), TURNS) + moves((7, 1), TURNS)
LAST = ((0, 4), (4, 8), (8, 32))


def mul(a, b):
    return lax.dot_general(a, b, (((1,), (0,)), ((), ())), precision=HIGHEST, preferred_element_type=F32)


def mul_t(a, b):
    return lax.dot_general(a, b, (((1,), (1,)), ((), ())), precision=HIGHEST, preferred_element_type=F32)


def swap_rows(a, b):
    low = lax.broadcasted_iota(jnp.int32, a.shape, a.ndim - 2) < 4
    return (
        jnp.where(low, a, pltpu.roll(b, 4, a.ndim - 2)),
        jnp.where(low, pltpu.roll(a, 4, a.ndim - 2), b),
    )


def polynomial(gram):
    side = gram.shape[0]
    eye = (
        lax.broadcasted_iota(jnp.int32, gram.shape, 0) == lax.broadcasted_iota(jnp.int32, gram.shape, 1)
    ).astype(F32)
    total = jnp.sum(jnp.sum(gram * eye, axis=1, keepdims=True), axis=0, keepdims=True)
    scale = lax.rsqrt(total + 1e-06)
    gram = (gram * scale) * scale
    factor = None
    for step in range(ITERS):
        now = 3.4445 * eye - 4.775 * gram + 2.0315 * mul(gram, gram)
        if step < ITERS - 1:
            gram = mul(mul(now, gram), now)
        factor = now if factor is None else mul(now, factor)
    return factor * scale


def kernel(n, chunks, grad_hbm, moment_hbm, weight_hbm, back, mom, weights, weight_sem, grads, moments, taken, made, wide, gram_own, gram_other,
           load_sem, send_sem, in_sem, gram_send_sem, gram_sem, back_sem,
           round_sem):
    me = lax.axis_index("fsdp")
    tp = lax.axis_index("tp")
    peer = 1 - tp

    def loads(m):
        rows = pl.ds(m * n, n)
        return (
            pltpu.make_async_copy(grad_hbm.at[rows], grads.at[rows], load_sem.at[0, m]),
            pltpu.make_async_copy(moment_hbm.at[rows], moments.at[rows], load_sem.at[1, m]),
        )

    for m in range(chunks):
        for copy in loads(m):
            copy.start()

    z, q = me // GROUP, me % GROUP
    odd = q % 2
    places = {OWN: 0, BESIDE: 1 + 2 * odd, ACROSS: 2, OBLIQUE: 3 - 2 * odd,
              FIRST: 2 * odd, SECOND: 2 - 2 * odd, THIRD: 1, FOURTH: 3}

    def at(dz, place):
        return lax.rem(z + dz, DEPTH) * GROUP + lax.rem(q + places[place], GROUP)

    barrier = pltpu.get_barrier_semaphore()
    greeted = moves((1, DEPTH - 1), ROW) + ((0, BESIDE), (0, ACROSS))
    for shift in greeted:
        pl.semaphore_signal(barrier, inc=1, device_id={"fsdp": at(*shift)}, device_id_type=MESH)
    pl.semaphore_signal(barrier, inc=1, device_id={"tp": peer}, device_id_type=MESH)

    def momentum(m):
        for copy in loads(m):
            copy.wait()
        rows = pl.ds(m * n, n)
        mom[rows] = hold_rate * moments[rows] + grads[rows]
        taken[m * n + me] = mom[m * n + me]

    def send(source, target, sem, m, to_shifts):
        for shift in to_shifts:
            to = at(*shift)
            pltpu.make_async_remote_copy(
                src_ref=source.at[m * n + to], dst_ref=target.at[m * n + me], send_sem=send_sem, recv_sem=sem.at[m],
                device_id={"fsdp": to}, device_id_type=MESH).start()

    def send_some(source, target, sem, m, to_moves, low, high):
        for move in to_moves:
            to = at(*move)

            @pl.when((to >= low) & (to < high))
            def _():
                pltpu.make_async_remote_copy(
                    src_ref=source.at[m * n + to], dst_ref=target.at[m * n + me], send_sem=send_sem,
                    recv_sem=sem.at[m], device_id={"fsdp": to}, device_id_type=MESH).start()

    def scatter(first, last, to_shifts):
        def one(m, carry):
            send(mom, taken, in_sem, m, to_shifts)
            return carry

        lax.fori_loop(first, last, one, 0)

    def round_of(step):
        told = ((1, OWN), (DEPTH - 1, OWN)) + (((0, ACROSS),) if step == 0 else ())
        for move in told:
            pl.semaphore_signal(round_sem.at[step], inc=1, device_id={"fsdp": at(*move)}, device_id_type=MESH)
        pl.semaphore_wait(round_sem.at[step], len(told))

    momentum(0)
    pl.semaphore_wait(barrier, len(greeted) + 1)
    for m in range(chunks):
        if m:
            momentum(m)
        send(mom, taken, in_sem, m, moves((1, 7), ROW) + ((0, BESIDE), (0, ACROSS)))
    round_of(0)
    scatter(0, chunks, moves((2, 6), ROW) + ((0, OBLIQUE),))
    round_of(1)
    round_of(2)
    round_of(3)
    scatter(0, chunks, moves((4, 3, 5), TURNS) + moves((2, 6, 1, 7), NEXT))
    def wait_for(buffer, sem, m):
        part = buffer.at[pl.ds(m * n, n - 1)]
        pltpu.make_async_copy(part, part, sem).wait()

    def compute(m, carry):
        wait_for(taken, in_sem.at[m], m)
        for j in range(4):
            block = taken[pl.ds(m * n, n), 8 * j:8 * j + 8, :].reshape(n // 2, 2, 8, 128)
            even, odd = swap_rows(block[:, 0], block[:, 1])
            wide[:, 256 * j:256 * j + 128] = even.reshape(4 * n, 128)
            wide[:, 256 * j + 128:256 * j + 256] = odd.reshape(4 * n, 128)
        gram_own[m] = mul_t(wide[...], wide[...])
        swap = pltpu.make_async_remote_copy(
            src_ref=gram_own.at[m], dst_ref=gram_other.at[m], send_sem=gram_send_sem.at[m], recv_sem=gram_sem.at[m],
            device_id={"tp": peer}, device_id_type=MESH)
        swap.start()
        swap.wait()
        factor = -learn_rate * polynomial(gram_own[m] + gram_other[m])
        for j in range(4):
            both = mul(factor, wide[:, 256 * j:256 * j + 256])
            a, b = swap_rows(both[:, :128].reshape(n // 2, 8, 128), both[:, 128:].reshape(n // 2, 8, 128))
            made[pl.ds(m * n, n), 8 * j:8 * j + 8, :] = jnp.stack([a, b], axis=1).reshape(n, 8, 128)
        back[m * n + me] = made[m * n + me]

        @pl.when(m < chunks - 1)
        def _():
            send(made, back, back_sem, m, OUT)

        @pl.when(m == chunks - 1)
        def _():
            for low, high in LAST:
                send_some(made, back, back_sem, m, OUT, low, high)

        return carry

    weight_load = pltpu.make_async_copy(weight_hbm, weights, weight_sem)
    weight_load.start()
    lax.fori_loop(0, chunks, compute, 0)
    weight_load.wait()
    for m in range(chunks):
        wait_for(back, back_sem.at[m], m)
        rows = pl.ds(m * n, n)
        back[rows] = weights[rows] + back[rows]
    for m in range(2 * chunks):
        wait_for(taken, send_sem, 0)


def finish(weight, mom, weight_out, mom_out, sem):
    copies = (pltpu.make_async_copy(weight, weight_out, sem.at[0]), pltpu.make_async_copy(mom, mom_out, sem.at[1]))
    for copy in copies:
        copy.start()
    for copy in copies:
        copy.wait()


def body(grad_stack, moment_stack, weight_stack):
    n = lax.axis_size("fsdp")
    mats, rows, cols = grad_stack.shape
    chunks = mats // n

    def tiles(x):
        return x.reshape(mats, rows, cols // 128, 128).transpose(0, 2, 1, 3).reshape(mats, rows * cols // 128, 128)

    def untiles(x):
        return x.reshape(mats, cols // 128, rows, 128).transpose(0, 2, 1, 3).reshape(mats, rows, cols)

    block = (mats, rows * cols // 128, 128)
    side = n * rows
    dma = pltpu.SemaphoreType.DMA
    back, momentum = pl.pallas_call(
        functools.partial(kernel, n, chunks),
        out_shape=[jax.ShapeDtypeStruct(block, F32)] * 2,
        in_specs=[pl.BlockSpec(memory_space=pltpu.HBM)] * 3,
        out_specs=[pl.BlockSpec(memory_space=pltpu.VMEM)] * 2,
        scratch_shapes=[
            pltpu.VMEM(block, F32), dma,
            pltpu.VMEM(block, F32), pltpu.VMEM(block, F32), pltpu.VMEM(block, F32), pltpu.VMEM(block, F32),
            pltpu.VMEM((side, cols), F32), pltpu.VMEM((chunks, side, side), F32), pltpu.VMEM((chunks, side, side), F32),
            dma((2, chunks)), dma, dma((chunks,)), dma((chunks,)), dma((chunks,)), dma((chunks,)),
            pltpu.SemaphoreType.REGULAR((4,)),
        ],
        compiler_params=pltpu.CompilerParams(collective_id=0, has_side_effects=True, vmem_limit_bytes=32 * 2**20),
    )(*(pltpu.with_memory_space_constraint(tiles(x), pltpu.HBM) for x in (grad_stack, moment_stack, weight_stack)))
    new_weights, new_momentum = pl.pallas_call(
        finish,
        out_shape=[jax.ShapeDtypeStruct(block, F32)] * 2,
        in_specs=[pl.BlockSpec(memory_space=pltpu.VMEM)] * 2,
        out_specs=[pl.BlockSpec(memory_space=pl.ANY)] * 2,
        scratch_shapes=[dma((2,))],
        compiler_params=pltpu.CompilerParams(vmem_limit_bytes=8 * 2**20),
    )(back, momentum)
    return (untiles(new_weights), untiles(new_momentum))


def solution(mesh):
    spec = P("shift", "fsdp", "tp")
    return jax.shard_map(body, mesh=mesh, in_specs=(spec,) * 3, out_specs=(spec,) * 2, check_vma=False)
```

```python
import functools

import jax
import jax.numpy as jnp
from jax import lax
from jax.experimental import pallas as pl
from jax.experimental.pallas import tpu as pltpu
from jax.sharding import PartitionSpec as P

ITERS = 3
DEPTH = 8
GROUP = 4
hold_rate = 0.95
learn_rate = 0.9

MESH = pl.DeviceIdType.MESH
HIGHEST = lax.Precision.HIGHEST
F32 = jnp.float32


OWN, BESIDE, ACROSS, OBLIQUE, FIRST, SECOND, THIRD, FOURTH = range(8)
ROW, NEXT, TURNS = (OWN, BESIDE), (ACROSS, OBLIQUE), (FIRST, SECOND, THIRD, FOURTH)
ZERO = ((0, BESIDE), (0, ACROSS), (0, OBLIQUE))


def moves(distances, places):
    return tuple((dz, place) for place in places for dz in distances)


OUT = moves((4,), TURNS) + moves((5, 3), TURNS) + moves((6, 2), TURNS) + moves((7, 1), TURNS) + ZERO
LAST = ((0, 4), (4, 8), (8, 32))


def mul(a, b):
    return lax.dot_general(a, b, (((1,), (0,)), ((), ())), precision=HIGHEST, preferred_element_type=F32)


def mul_t(a, b):
    return lax.dot_general(a, b, (((1,), (1,)), ((), ())), precision=HIGHEST, preferred_element_type=F32)


def swap_rows(a, b):
    low = lax.broadcasted_iota(jnp.int32, a.shape, a.ndim - 2) < 4
    return (
        jnp.where(low, a, pltpu.roll(b, 4, a.ndim - 2)),
        jnp.where(low, pltpu.roll(a, 4, a.ndim - 2), b),
    )


def polynomial(gram):
    side = gram.shape[0]
    eye = (
        lax.broadcasted_iota(jnp.int32, gram.shape, 0) == lax.broadcasted_iota(jnp.int32, gram.shape, 1)
    ).astype(F32)
    total = jnp.sum(jnp.sum(gram * eye, axis=1, keepdims=True), axis=0, keepdims=True)
    scale = lax.rsqrt(total + 1e-06)
    gram = (gram * scale) * scale
    factor = None
    for step in range(ITERS):
        now = 3.4445 * eye - 4.775 * gram + 2.0315 * mul(gram, gram)
        if step < ITERS - 1:
            gram = mul(mul(now, gram), now)
        factor = now if factor is None else mul(now, factor)
    return factor * scale


def kernel(n, chunks, grad_hbm, moment_hbm, back, mom, grads, moments, taken, made, wide, gram_own, gram_other,
           load_sem, send_sem, in_sem, gram_send_sem, gram_sem, back_sem,
           round_sem):
    me = lax.axis_index("fsdp")
    tp = lax.axis_index("tp")
    peer = 1 - tp

    def loads(m):
        rows = pl.ds(m * n, n)
        return (
            pltpu.make_async_copy(grad_hbm.at[rows], grads.at[rows], load_sem.at[0, m]),
            pltpu.make_async_copy(moment_hbm.at[rows], moments.at[rows], load_sem.at[1, m]),
        )

    for m in range(chunks):
        for copy in loads(m):
            copy.start()

    z, q = me // GROUP, me % GROUP
    odd = q % 2
    places = {OWN: 0, BESIDE: 1 + 2 * odd, ACROSS: 2, OBLIQUE: 3 - 2 * odd,
              FIRST: 2 * odd, SECOND: 2 - 2 * odd, THIRD: 1, FOURTH: 3}

    def at(dz, place):
        return lax.rem(z + dz, DEPTH) * GROUP + lax.rem(q + places[place], GROUP)

    barrier = pltpu.get_barrier_semaphore()
    greeted = moves((1, DEPTH - 1), ROW) + ((0, BESIDE), (0, ACROSS))
    for shift in greeted:
        pl.semaphore_signal(barrier, inc=1, device_id={"fsdp": at(*shift)}, device_id_type=MESH)
    pl.semaphore_signal(barrier, inc=1, device_id={"tp": peer}, device_id_type=MESH)

    def momentum(m):
        for copy in loads(m):
            copy.wait()
        rows = pl.ds(m * n, n)
        mom[rows] = hold_rate * moments[rows] + grads[rows]
        taken[m * n + me] = mom[m * n + me]

    def send(source, target, sem, m, to_shifts):
        for shift in to_shifts:
            to = at(*shift)
            pltpu.make_async_remote_copy(
                src_ref=source.at[m * n + to], dst_ref=target.at[m * n + me], send_sem=send_sem, recv_sem=sem.at[m],
                device_id={"fsdp": to}, device_id_type=MESH).start()

    def send_some(source, target, sem, m, to_moves, low, high):
        for move in to_moves:
            to = at(*move)

            @pl.when((to >= low) & (to < high))
            def _():
                pltpu.make_async_remote_copy(
                    src_ref=source.at[m * n + to], dst_ref=target.at[m * n + me], send_sem=send_sem,
                    recv_sem=sem.at[m], device_id={"fsdp": to}, device_id_type=MESH).start()

    def scatter(first, last, to_shifts):
        def one(m, carry):
            send(mom, taken, in_sem, m, to_shifts)
            return carry

        lax.fori_loop(first, last, one, 0)

    def round_of(step):
        told = ((1, OWN), (DEPTH - 1, OWN)) + (((0, ACROSS),) if step == 0 else ())
        for move in told:
            pl.semaphore_signal(round_sem.at[step], inc=1, device_id={"fsdp": at(*move)}, device_id_type=MESH)
        pl.semaphore_wait(round_sem.at[step], len(told))

    momentum(0)
    pl.semaphore_wait(barrier, len(greeted) + 1)
    for m in range(chunks):
        if m:
            momentum(m)
        send(mom, taken, in_sem, m, moves((1, 7), ROW) + ((0, BESIDE), (0, ACROSS)))
    round_of(0)
    scatter(0, chunks, moves((2, 6), ROW) + ((0, OBLIQUE),))
    round_of(1)
    round_of(2)
    round_of(3)
    scatter(0, chunks, moves((4, 3, 5), TURNS) + moves((2, 6, 1, 7), NEXT))
    def wait_for(buffer, sem, m):
        part = buffer.at[pl.ds(m * n, n - 1)]
        pltpu.make_async_copy(part, part, sem).wait()

    def compute(m, carry):
        wait_for(taken, in_sem.at[m], m)
        for j in range(4):
            block = taken[pl.ds(m * n, n), 8 * j:8 * j + 8, :].reshape(n // 2, 2, 8, 128)
            even, odd = swap_rows(block[:, 0], block[:, 1])
            wide[:, 256 * j:256 * j + 128] = even.reshape(4 * n, 128)
            wide[:, 256 * j + 128:256 * j + 256] = odd.reshape(4 * n, 128)
        gram_own[m] = mul_t(wide[...], wide[...])
        swap = pltpu.make_async_remote_copy(
            src_ref=gram_own.at[m], dst_ref=gram_other.at[m], send_sem=gram_send_sem.at[m], recv_sem=gram_sem.at[m],
            device_id={"tp": peer}, device_id_type=MESH)
        swap.start()
        swap.wait()
        factor = -learn_rate * polynomial(gram_own[m] + gram_other[m])
        for j in range(4):
            both = mul(factor, wide[:, 256 * j:256 * j + 256])
            a, b = swap_rows(both[:, :128].reshape(n // 2, 8, 128), both[:, 128:].reshape(n // 2, 8, 128))
            made[pl.ds(m * n, n), 8 * j:8 * j + 8, :] = jnp.stack([a, b], axis=1).reshape(n, 8, 128)
        back[m * n + me] = made[m * n + me]

        @pl.when(m < chunks - 1)
        def _():
            send(made, back, back_sem, m, OUT)

        @pl.when(m == chunks - 1)
        def _():
            for low, high in LAST:
                send_some(made, back, back_sem, m, OUT, low, high)

        return carry

    lax.fori_loop(0, chunks, compute, 0)
    for m in range(chunks):
        wait_for(back, back_sem.at[m], m)
    for m in range(2 * chunks):
        wait_for(taken, send_sem, 0)


def finish(parts, weight, back, mom, weight_out, mom_out, total, sem):
    copies = [pltpu.make_async_copy(mom, mom_out, sem.at[parts])]
    copies[0].start()
    size = weight.shape[0] // parts
    for i in range(parts):
        rows = pl.ds(i * size, size)
        total[rows] = weight[rows] + back[rows]
        copies.append(pltpu.make_async_copy(total.at[rows], weight_out.at[rows], sem.at[i]))
        copies[-1].start()
    for copy in copies:
        copy.wait()


def body(grad_stack, moment_stack, weight_stack):
    n = lax.axis_size("fsdp")
    mats, rows, cols = grad_stack.shape
    chunks = mats // n

    def tiles(x):
        return x.reshape(mats, rows, cols // 128, 128).transpose(0, 2, 1, 3).reshape(mats, rows * cols // 128, 128)

    def untiles(x):
        return x.reshape(mats, cols // 128, rows, 128).transpose(0, 2, 1, 3).reshape(mats, rows, cols)

    block = (mats, rows * cols // 128, 128)
    side = n * rows
    dma = pltpu.SemaphoreType.DMA
    back, momentum = pl.pallas_call(
        functools.partial(kernel, n, chunks),
        out_shape=[jax.ShapeDtypeStruct(block, F32)] * 2,
        in_specs=[pl.BlockSpec(memory_space=pltpu.HBM)] * 2,
        out_specs=[pl.BlockSpec(memory_space=pltpu.VMEM)] * 2,
        scratch_shapes=[
            pltpu.VMEM(block, F32), pltpu.VMEM(block, F32), pltpu.VMEM(block, F32), pltpu.VMEM(block, F32),
            pltpu.VMEM((side, cols), F32), pltpu.VMEM((chunks, side, side), F32), pltpu.VMEM((chunks, side, side), F32),
            dma((2, chunks)), dma, dma((chunks,)), dma((chunks,)), dma((chunks,)), dma((chunks,)),
            pltpu.SemaphoreType.REGULAR((4,)),
        ],
        compiler_params=pltpu.CompilerParams(collective_id=0, has_side_effects=True, vmem_limit_bytes=32 * 2**20),
    )(*(pltpu.with_memory_space_constraint(tiles(x), pltpu.HBM) for x in (grad_stack, moment_stack)))
    new_weights, new_momentum = pl.pallas_call(
        functools.partial(finish, 4),
        out_shape=[jax.ShapeDtypeStruct(block, F32)] * 2,
        in_specs=[pl.BlockSpec(memory_space=pltpu.VMEM)] * 3,
        out_specs=[pl.BlockSpec(memory_space=pl.ANY)] * 2,
        scratch_shapes=[pltpu.VMEM(block, F32), dma((5,))],
        compiler_params=pltpu.CompilerParams(vmem_limit_bytes=8 * 2**20),
    )(tiles(weight_stack), back, momentum)
    return (untiles(new_weights), untiles(new_momentum))


def solution(mesh):
    spec = P("shift", "fsdp", "tp")
    return jax.shard_map(body, mesh=mesh, in_specs=(spec,) * 3, out_specs=(spec,) * 2, check_vma=False)
```

```python
import functools

import jax
import jax.numpy as jnp
from jax import lax
from jax.experimental import pallas as pl
from jax.experimental.pallas import tpu as pltpu
from jax.sharding import PartitionSpec as P

ITERS = 3
DEPTH = 8
GROUP = 4
hold_rate = 0.95
learn_rate = 0.9

MESH = pl.DeviceIdType.MESH
HIGHEST = lax.Precision.HIGHEST
F32 = jnp.float32


OWN, BESIDE, ACROSS, OBLIQUE, FIRST, SECOND, THIRD, FOURTH = range(8)
ROW, NEXT, TURNS = (OWN, BESIDE), (ACROSS, OBLIQUE), (FIRST, SECOND, THIRD, FOURTH)
ZERO = ((0, BESIDE), (0, ACROSS), (0, OBLIQUE))


def moves(distances, places):
    return tuple((dz, place) for place in places for dz in distances)


OUT = ZERO + moves((4,), TURNS) + moves((5, 3), TURNS) + moves((6, 2), TURNS) + moves((7, 1), TURNS)
LAST = ((0, 4), (4, 8), (8, 10), (10, 32))


def mul(a, b):
    return lax.dot_general(a, b, (((1,), (0,)), ((), ())), precision=HIGHEST, preferred_element_type=F32)


def mul_t(a, b):
    return lax.dot_general(a, b, (((1,), (1,)), ((), ())), precision=HIGHEST, preferred_element_type=F32)


def swap_rows(a, b):
    low = lax.broadcasted_iota(jnp.int32, a.shape, a.ndim - 2) < 4
    return (
        jnp.where(low, a, pltpu.roll(b, 4, a.ndim - 2)),
        jnp.where(low, pltpu.roll(a, 4, a.ndim - 2), b),
    )


def polynomial(gram):
    side = gram.shape[0]
    eye = (
        lax.broadcasted_iota(jnp.int32, gram.shape, 0) == lax.broadcasted_iota(jnp.int32, gram.shape, 1)
    ).astype(F32)
    total = jnp.sum(jnp.sum(gram * eye, axis=1, keepdims=True), axis=0, keepdims=True)
    scale = lax.rsqrt(total + 1e-06)
    gram = (gram * scale) * scale
    factor = None
    for step in range(ITERS):
        now = 3.4445 * eye - 4.775 * gram + 2.0315 * mul(gram, gram)
        if step < ITERS - 1:
            gram = mul(mul(now, gram), now)
        factor = now if factor is None else mul(now, factor)
    return factor * scale


def kernel(n, chunks, grad_hbm, moment_hbm, back, mom, grads, moments, taken, made, wide, gram_own, gram_other,
           load_sem, send_sem, in_sem, gram_send_sem, gram_sem, back_sem,
           round_sem):
    me = lax.axis_index("fsdp")
    tp = lax.axis_index("tp")
    peer = 1 - tp

    def loads(m):
        rows = pl.ds(m * n, n)
        return (
            pltpu.make_async_copy(grad_hbm.at[rows], grads.at[rows], load_sem.at[0, m]),
            pltpu.make_async_copy(moment_hbm.at[rows], moments.at[rows], load_sem.at[1, m]),
        )

    for m in range(chunks):
        for copy in loads(m):
            copy.start()

    z, q = me // GROUP, me % GROUP
    odd = q % 2
    places = {OWN: 0, BESIDE: 1 + 2 * odd, ACROSS: 2, OBLIQUE: 3 - 2 * odd,
              FIRST: 2 * odd, SECOND: 2 - 2 * odd, THIRD: 1, FOURTH: 3}

    def at(dz, place):
        return lax.rem(z + dz, DEPTH) * GROUP + lax.rem(q + places[place], GROUP)

    barrier = pltpu.get_barrier_semaphore()
    greeted = moves((1, DEPTH - 1), ROW) + ((0, BESIDE), (0, ACROSS))
    for shift in greeted:
        pl.semaphore_signal(barrier, inc=1, device_id={"fsdp": at(*shift)}, device_id_type=MESH)
    pl.semaphore_signal(barrier, inc=1, device_id={"tp": peer}, device_id_type=MESH)

    def momentum(m):
        for copy in loads(m):
            copy.wait()
        rows = pl.ds(m * n, n)
        mom[rows] = hold_rate * moments[rows] + grads[rows]
        taken[m * n + me] = mom[m * n + me]

    def send(source, target, sem, m, to_shifts):
        for shift in to_shifts:
            to = at(*shift)
            pltpu.make_async_remote_copy(
                src_ref=source.at[m * n + to], dst_ref=target.at[m * n + me], send_sem=send_sem, recv_sem=sem.at[m],
                device_id={"fsdp": to}, device_id_type=MESH).start()

    def send_some(source, target, sem, m, to_moves, low, high):
        for move in to_moves:
            to = at(*move)

            @pl.when((to >= low) & (to < high))
            def _():
                pltpu.make_async_remote_copy(
                    src_ref=source.at[m * n + to], dst_ref=target.at[m * n + me], send_sem=send_sem,
                    recv_sem=sem.at[m], device_id={"fsdp": to}, device_id_type=MESH).start()

    def scatter(first, last, to_shifts):
        def one(m, carry):
            send(mom, taken, in_sem, m, to_shifts)
            return carry

        lax.fori_loop(first, last, one, 0)

    def round_of(step):
        told = ((1, OWN), (DEPTH - 1, OWN)) + (((0, ACROSS),) if step == 0 else ())
        for move in told:
            pl.semaphore_signal(round_sem.at[step], inc=1, device_id={"fsdp": at(*move)}, device_id_type=MESH)
        pl.semaphore_wait(round_sem.at[step], len(told))

    momentum(0)
    pl.semaphore_wait(barrier, len(greeted) + 1)
    for m in range(chunks):
        if m:
            momentum(m)
        send(mom, taken, in_sem, m, moves((1, 7), ROW) + ((0, BESIDE), (0, ACROSS)))
    round_of(0)
    scatter(0, chunks, moves((2, 6), ROW) + ((0, OBLIQUE),))
    round_of(1)
    round_of(2)
    round_of(3)
    scatter(0, chunks, moves((4, 3, 5), TURNS) + moves((2, 6, 1, 7), NEXT))
    def wait_for(buffer, sem, m):
        part = buffer.at[pl.ds(m * n, n - 1)]
        pltpu.make_async_copy(part, part, sem).wait()

    def compute(m, carry):
        wait_for(taken, in_sem.at[m], m)
        for j in range(4):
            block = taken[pl.ds(m * n, n), 8 * j:8 * j + 8, :].reshape(n // 2, 2, 8, 128)
            even, odd = swap_rows(block[:, 0], block[:, 1])
            wide[:, 256 * j:256 * j + 128] = even.reshape(4 * n, 128)
            wide[:, 256 * j + 128:256 * j + 256] = odd.reshape(4 * n, 128)
        gram_own[m] = mul_t(wide[...], wide[...])
        swap = pltpu.make_async_remote_copy(
            src_ref=gram_own.at[m], dst_ref=gram_other.at[m], send_sem=gram_send_sem.at[m], recv_sem=gram_sem.at[m],
            device_id={"tp": peer}, device_id_type=MESH)
        swap.start()
        swap.wait()
        factor = -learn_rate * polynomial(gram_own[m] + gram_other[m])
        for j in range(4):
            both = mul(factor, wide[:, 256 * j:256 * j + 256])
            a, b = swap_rows(both[:, :128].reshape(n // 2, 8, 128), both[:, 128:].reshape(n // 2, 8, 128))
            made[pl.ds(m * n, n), 8 * j:8 * j + 8, :] = jnp.stack([a, b], axis=1).reshape(n, 8, 128)
        back[m * n + me] = made[m * n + me]

        @pl.when(m < chunks - 1)
        def _():
            send(made, back, back_sem, m, OUT)

        @pl.when(m == chunks - 1)
        def _():
            for low, high in LAST:
                send_some(made, back, back_sem, m, OUT, low, high)

        return carry

    lax.fori_loop(0, chunks, compute, 0)
    for m in range(chunks):
        wait_for(back, back_sem.at[m], m)
    for m in range(2 * chunks):
        wait_for(taken, send_sem, 0)


def finish(parts, weight, back, mom, weight_out, mom_out, total, sem):
    copies = [pltpu.make_async_copy(mom, mom_out, sem.at[parts])]
    copies[0].start()
    size = weight.shape[0] // parts
    for i in range(parts):
        rows = pl.ds(i * size, size)
        total[rows] = weight[rows] + back[rows]
        copies.append(pltpu.make_async_copy(total.at[rows], weight_out.at[rows], sem.at[i]))
        copies[-1].start()
    for copy in copies:
        copy.wait()


def body(grad_stack, moment_stack, weight_stack):
    n = lax.axis_size("fsdp")
    mats, rows, cols = grad_stack.shape
    chunks = mats // n

    def tiles(x):
        return x.reshape(mats, rows, cols // 128, 128).transpose(0, 2, 1, 3).reshape(mats, rows * cols // 128, 128)

    def untiles(x):
        return x.reshape(mats, cols // 128, rows, 128).transpose(0, 2, 1, 3).reshape(mats, rows, cols)

    block = (mats, rows * cols // 128, 128)
    side = n * rows
    dma = pltpu.SemaphoreType.DMA
    back, momentum = pl.pallas_call(
        functools.partial(kernel, n, chunks),
        out_shape=[jax.ShapeDtypeStruct(block, F32)] * 2,
        in_specs=[pl.BlockSpec(memory_space=pltpu.HBM)] * 2,
        out_specs=[pl.BlockSpec(memory_space=pltpu.VMEM)] * 2,
        scratch_shapes=[
            pltpu.VMEM(block, F32), pltpu.VMEM(block, F32), pltpu.VMEM(block, F32), pltpu.VMEM(block, F32),
            pltpu.VMEM((side, cols), F32), pltpu.VMEM((chunks, side, side), F32), pltpu.VMEM((chunks, side, side), F32),
            dma((2, chunks)), dma, dma((chunks,)), dma((chunks,)), dma((chunks,)), dma((chunks,)),
            pltpu.SemaphoreType.REGULAR((4,)),
        ],
        compiler_params=pltpu.CompilerParams(collective_id=0, has_side_effects=True, vmem_limit_bytes=32 * 2**20),
    )(*(pltpu.with_memory_space_constraint(tiles(x), pltpu.HBM) for x in (grad_stack, moment_stack)))
    new_weights, new_momentum = pl.pallas_call(
        functools.partial(finish, 4),
        out_shape=[jax.ShapeDtypeStruct(block, F32)] * 2,
        in_specs=[pl.BlockSpec(memory_space=pltpu.VMEM)] * 3,
        out_specs=[pl.BlockSpec(memory_space=pl.ANY)] * 2,
        scratch_shapes=[pltpu.VMEM(block, F32), dma((5,))],
        compiler_params=pltpu.CompilerParams(vmem_limit_bytes=8 * 2**20),
    )(tiles(weight_stack), back, momentum)
    return (untiles(new_weights), untiles(new_momentum))


def solution(mesh):
    spec = P("shift", "fsdp", "tp")
    return jax.shard_map(body, mesh=mesh, in_specs=(spec,) * 3, out_specs=(spec,) * 2, check_vma=False)
```
